32 devices in a mesh: expert: 4 (over y, core), fsdp: 8 (over z, x).
Axes of the slice: x: 2, y: 2, z: 4, core: 2. Of those that a mesh axis runs over, the one named last changes fastest.
Arguments:
- gradients: bfloat16 [8, 3584, 1024], P('expert', 'fsdp'), may hold values from -24 to 24, as said below
- owner: int32 [4, 2], P('expert'), may hold values from 0 to 1, each once within a row
Outputs:
- updates: bfloat16 [8, 3584, 1024], P('expert', 'fsdp')
- slot_rms: float32 [4, 8], P('expert', 'fsdp')
The draws below stay inside these ranges and needn't reach their ends.
Inputs may be any that keep to these rules, and one draw needn't show every extreme that they name: gradients are values of mean zero and unit variance times a factor per expert between 0.5 and 2 and a factor per expert and row slice between 0.5 and 2, each entry within 24 in magnitude. Each row of owner names every place 0 to 1 exactly once.
All inputs are finite; a program needn't handle non-finite values.
Results may differ from the reference program's by a relative error of at most 0.009.
Values may be sent and summed in bfloat16 or wider, within the bound.
A program may use at most 64 MiB of HBM per device.

```python
import math
import jax
import jax.numpy as jnp
from jax import lax

ROWS = 3584
COLS = 1024
SHARE = 4
ITERS = 3
EXP_GROUP = 2
GROUPS = 4
EXPERTS = 8
N_FSDP = 8


def draw_gradients(key, part):
    scale_key, slice_key, value_key = jax.random.split(jax.random.fold_in(key, 11), 3)
    scales = jnp.exp(jax.random.uniform(scale_key, (EXPERTS, 1, 1), jnp.float32, math.log(0.5), math.log(2.0)))
    slice_scales = jnp.exp(jax.random.uniform(slice_key, (EXPERTS, SHARE), jnp.float32, math.log(0.5), math.log(2.0)))
    row_index = jnp.arange(ROWS, dtype=jnp.int32)
    slice_index = row_index % (ROWS // N_FSDP) // (ROWS // N_FSDP // SHARE)
    row_scales = jnp.take(slice_scales, slice_index, axis=1)[:, :, None]
    values = jnp.clip(jax.random.normal(value_key, (EXPERTS, ROWS, COLS), jnp.float32), -6.0, 6.0)
    return (values * scales * row_scales).astype(jnp.bfloat16)


def setup_inputs(seed: int = 0) -> dict:
    key_list = jax.random.split(jax.random.key(seed), 3)
    return {
        "gradients": draw_gradients(jax.random.fold_in(key_list[2], 71), 0),
        "owner": jax.vmap(lambda own: jax.random.permutation(own, EXP_GROUP))(jax.random.split(key_list[1], GROUPS)).reshape((GROUPS, EXP_GROUP)).astype(jnp.int32),
    }


coef_a = 3.4445
coef_b = -4.775
coef_c = 2.0315
epsilon = 1e-07

def orthogonalize(matrix):
    grad_float = matrix.astype(jnp.float32)
    square_sum = jnp.sum(grad_float * grad_float)
    norm_value = jnp.sqrt(square_sum)
    current = (grad_float / (norm_value + epsilon)).astype(jnp.bfloat16)
    per_slice = ROWS // N_FSDP // SHARE
    for iteration in range(ITERS):
        row_blocks = current.reshape(N_FSDP, SHARE, per_slice, COLS)
        gram_sum = jnp.zeros((COLS, COLS), jnp.float32)
        for portion in range(SHARE):
            slice_rows = row_blocks[:, portion].reshape(N_FSDP * per_slice, COLS)
            partial_gram = jnp.dot(slice_rows.T, slice_rows, preferred_element_type=jnp.float32)
            rounded = lax.optimization_barrier(partial_gram.astype(jnp.bfloat16))
            gram_sum = gram_sum + rounded.astype(jnp.float32)
        gram_full = lax.optimization_barrier(gram_sum.astype(jnp.bfloat16))
        squared = jnp.dot(gram_full, gram_full, preferred_element_type=jnp.float32)
        poly = (coef_b * gram_full.astype(jnp.float32) + coef_c * squared).astype(jnp.bfloat16)
        current = (coef_a * current.astype(jnp.float32) + jnp.dot(current, poly, preferred_element_type=jnp.float32)).astype(jnp.bfloat16)
    update = (math.sqrt(ROWS) * current.astype(jnp.float32)).astype(jnp.bfloat16)
    rms_value = norm_value / math.sqrt(ROWS * COLS)
    return (update, rms_value)

def reference(gradients, owner):
    updates, rms_values = lax.map(orthogonalize, gradients)
    rms_grid = rms_values.reshape(GROUPS, EXP_GROUP)
    places = jnp.arange(EXP_GROUP, dtype=jnp.int32)
    onehot = (owner[:, :, None] == places[None, None, :]).astype(jnp.float32)
    slot_values = lax.optimization_barrier(jnp.sum(onehot * rms_grid[:, :, None], axis=1))
    slot_rms = jnp.repeat(slot_values, SHARE, axis=1)
    return (updates, slot_rms)
```

```python
import math

import jax
import jax.numpy as jnp
from jax import lax
from jax.sharding import PartitionSpec as P

coef_a = 3.4445
coef_b = -4.775
coef_c = 2.0315
epsilon = 1e-07
ITERS = 3


def mm(a, b):
    return jnp.dot(a, b, preferred_element_type=jnp.float32)


def body(gradients, owner):
    expert_count, local_rows, columns = gradients.shape
    fsdp_size = lax.axis_size("fsdp")
    rows = local_rows * fsdp_size
    share = fsdp_size // expert_count
    f32, bf16 = jnp.float32, jnp.bfloat16
    sums = jnp.sum(jnp.square(gradients.astype(f32)), axis=(1, 2))
    totals = lax.psum(sums, "fsdp")
    norms = jnp.sqrt(totals)
    scales = 1.0 / (norms + epsilon)

    def one(pair):
        g, scale = pair
        local = lax.dot_general(g, g, (((0,), (0,)), ((), ())), preferred_element_type=f32)
        raw = lax.psum(local.astype(bf16), "fsdp")
        gram = (raw.astype(f32) * (scale * scale)).astype(bf16)
        current = g
        for it in range(ITERS):
            gf = gram.astype(f32)
            poly = (coef_b * gf + coef_c * mm(gram, gram)).astype(bf16)
            nxt = coef_a * current.astype(f32) + mm(current, poly)
            if it == 0:
                nxt = nxt * scale
            if it < ITERS - 1:
                half = (coef_a * gf + mm(gram, poly)).astype(bf16)
                gram = (coef_a * half.astype(f32) + mm(poly, half)).astype(bf16)
                current = nxt.astype(bf16)
        return (math.sqrt(rows) * nxt).astype(bf16)

    if expert_count <= 2:
        updates = jnp.stack([one((gradients[e], scales[e])) for e in range(expert_count)])
    else:
        updates = lax.map(one, (gradients, scales))
    place = lax.axis_index("fsdp") // share
    mine = jnp.sum(jnp.where(owner[0] == place, norms, 0.0))
    slot_rms = (mine / math.sqrt(rows * columns)).reshape(1, 1)
    return updates, slot_rms


def solution(mesh):
    return jax.shard_map(
        body,
        mesh=mesh,
        in_specs=(P("expert", "fsdp", None), P("expert", None)),
        out_specs=(P("expert", "fsdp", None), P("expert", "fsdp")),
        check_vma=False,
    )
```

```python
import functools
import math

import jax
import jax.numpy as jnp
from jax import lax
from jax.experimental import pallas as pl
from jax.experimental.pallas import tpu as pltpu
from jax.sharding import PartitionSpec as P

coef_a = 3.4445
coef_b = -4.775
coef_c = 2.0315
epsilon = 1e-07
ITERS = 3
MESH = pl.DeviceIdType.MESH
f32, bf16 = jnp.float32, jnp.bfloat16


def mm(a, b):
    return jnp.dot(a, b, preferred_element_type=f32)


def kernel(rows, g_ref, out_ref, norm_ref, part, xr, pair, zr, red, gram, poly, half, ping, pong, nb,
           n_send, n_recv, xs_send, xs_recv, zs_send, zs_recv, za_send, za_recv, xa_send, xa_recv):
    experts, local_rows, columns = g_ref.shape
    tile = columns // 4
    piece = tile // 4
    blocks = [(i, j) for i in range(4) for j in range(i, 4)]
    per = len(blocks) // 2
    chunks = experts * per
    size = lax.axis_size("fsdp")
    me = lax.axis_index("fsdp")
    z, x = me // 2, me % 2
    partner = z * 2 + (1 - x)

    barrier = pltpu.get_barrier_semaphore()
    for d in range(1, size):
        pl.semaphore_signal(barrier, inc=1, device_id={"fsdp": (me + d) % size}, device_id_type=MESH)

    def remote(src, dst, send, recv, peer):
        return pltpu.make_async_remote_copy(
            src_ref=src, dst_ref=dst, send_sem=send, recv_sem=recv, device_id={"fsdp": peer}, device_id_type=MESH
        )

    def local_gram(e):
        for i in range(4):
            strip = lax.dot_general(
                g_ref[e, :, tile * i:tile * (i + 1)], g_ref[e, :, tile * i:], (((0,), (0,)), ((), ())),
                preferred_element_type=f32,
            ).astype(bf16)
            for j in range(i, 4):
                part[e, blocks.index((i, j))] = strip[:, tile * (j - i):tile * (j - i + 1)]

    def squares(e):
        total = jnp.zeros((8, 128), f32)
        for n in range(columns // 128):
            value = g_ref[e, :, 128 * n:128 * (n + 1)].astype(f32)
            total = total + jnp.sum((value * value).reshape(local_rows // 8, 8, 128), axis=0)
        nb[0, e] = total

    def x_scatter(k):
        e, c = divmod(k, per)
        return remote(part.at[e, per * (1 - x) + c], xr.at[k], xs_send.at[k], xs_recv.at[k], partner)

    def z_peer(d):
        return (z + d) % 4

    def z_scatter(k, d):
        rows_of = pl.ds(pl.multiple_of(z_peer(d) * piece, piece), piece)
        return remote(pair.at[k, rows_of], zr.at[k, d - 1], zs_send.at[k, d - 1], zs_recv.at[k, d - 1],
                      z_peer(d) * 2 + x)

    mine = pl.ds(pl.multiple_of(z * piece, piece), piece)

    def z_gather(k, d):
        e, c = divmod(k, per)
        slot = red.at[e, per * x + c, mine]
        return remote(slot, slot, za_send.at[k, d - 1], za_recv.at[k, d - 1], z_peer(d) * 2 + x)

    def x_gather(k):
        e, c = divmod(k, per)
        slot = red.at[e, per * x + c]
        return remote(slot, slot, xa_send.at[k], xa_recv.at[k], partner)

    def step_b(k):
        e, c = divmod(k, per)
        x_scatter(k).wait_recv()
        pair[k] = (part[e, per * x + c].astype(f32) + xr[k].astype(f32)).astype(bf16)
        for d in (2, 1, 3):
            z_scatter(k, d).start()

    def step_c(k):
        e, c = divmod(k, per)
        total = pair[k, mine].astype(f32)
        for d in (1, 2, 3):
            z_scatter(k, d).wait_recv()
            total = total + zr[k, d - 1].astype(f32)
        red[e, per * x + c, mine] = total.astype(bf16)
        for d in (2, 1, 3):
            z_gather(k, d).start()

    def step_d(k):
        for d in (1, 2, 3):
            z_gather(k, d).wait_recv()
        x_gather(k).start()
        if k + per < chunks:
            x_scatter(k + per).start()

    def unpack(e, scale):
        for c in range(per):
            x_gather(e * per + c).wait_recv()
        for b, (i, j) in enumerate(blocks):
            block = red[e, b].astype(f32) * (scale * scale)
            gram[tile * i:tile * (i + 1), tile * j:tile * (j + 1)] = block.astype(bf16)
            if i != j:
                gram[tile * j:tile * (j + 1), tile * i:tile * (i + 1)] = block.T.astype(bf16)

    def by_columns(fn):
        def step(n, carry):
            fn(pl.ds(pl.multiple_of(n * tile, tile), tile))
            return carry
        lax.fori_loop(0, 4, step, 0)

    def stage_poly():
        def fn(cols):
            poly[:, cols] = (coef_b * gram[:, cols].astype(f32) + coef_c * mm(gram[...], gram[:, cols])).astype(bf16)
        by_columns(fn)

    def stage_half():
        def fn(cols):
            half[:, cols] = (coef_a * gram[:, cols].astype(f32) + mm(gram[...], poly[:, cols])).astype(bf16)
        by_columns(fn)

    def stage_gram():
        def fn(cols):
            gram[:, cols] = (coef_a * half[:, cols].astype(f32) + mm(poly[...], half[:, cols])).astype(bf16)
        by_columns(fn)

    def stage_rows(src, dst, factor):
        def fn(cols):
            value = coef_a * src[:, cols].astype(f32) + mm(src[...], poly[:, cols])
            if factor is not None:
                value = value * factor
            dst[:, cols] = value.astype(bf16)
        by_columns(fn)

    def stages(e, scale):
        root = math.sqrt(rows)
        return [
            functools.partial(unpack, e, scale),
            stage_poly, stage_half, stage_gram,
            functools.partial(stage_rows, g_ref.at[e], ping, scale),
            stage_poly, stage_half, stage_gram,
            functools.partial(stage_rows, ping, pong, None),
            stage_poly,
            functools.partial(stage_rows, pong, out_ref.at[e], root),
        ]

    local_gram(0)
    pl.semaphore_wait(barrier, size - 1)
    for k in range(per):
        x_scatter(k).start()
    for e in range(experts):
        squares(e)

    def norm_copy(d):
        return remote(nb.at[0], nb.at[d], n_send.at[d - 1], n_recv.at[d - 1], (me + d) % size)

    for d in range(1, size):
        norm_copy(d).start()
    local_gram(1)

    scales = []

    def finish_norms():
        total = nb[0]
        for d in range(1, size):
            norm_copy(d).wait_recv()
            total = total + nb[d]
        for e in range(experts):
            norm = jnp.sqrt(jnp.sum(total[e], keepdims=True))
            norm_ref[e] = jnp.broadcast_to(norm, (8, 128))
            scales.append(1.0 / (norm + epsilon))

    work = []
    for t in range(chunks + 2):
        if t < chunks:
            step_b(t)
        if 0 <= t - 1 < chunks:
            step_c(t - 1)
        if 0 <= t - 2 < chunks:
            step_d(t - 2)
        if t == per:
            finish_norms()
            work = stages(0, scales[0])
        if t >= per + 2:
            for _ in range(3):
                if work:
                    work.pop(0)()
    while work:
        work.pop(0)()
    for stage in stages(1, scales[1]):
        stage()

    for k in range(chunks):
        x_scatter(k).wait_send()
        x_gather(k).wait_send()
        for d in (1, 2, 3):
            z_scatter(k, d).wait_send()
            z_gather(k, d).wait_send()
    for d in range(1, size):
        norm_copy(d).wait_send()


def fused(gradients, rows):
    experts, local_rows, columns = gradients.shape
    tile = columns // 4
    chunks = experts * 5
    dma = pltpu.SemaphoreType.DMA
    vmem = pl.BlockSpec(memory_space=pltpu.VMEM)
    return pl.pallas_call(
        functools.partial(kernel, rows),
        out_shape=(
            jax.ShapeDtypeStruct(gradients.shape, bf16),
            jax.ShapeDtypeStruct((experts, 8, 128), f32),
        ),
        in_specs=[vmem],
        out_specs=(vmem, vmem),
        scratch_shapes=[
            pltpu.VMEM((experts, 10, tile, tile), bf16),
            pltpu.VMEM((chunks, tile, tile), bf16),
            pltpu.VMEM((chunks, tile, tile), bf16),
            pltpu.VMEM((chunks, 3, tile // 4, tile), bf16),
            pltpu.VMEM((experts, 10, tile, tile), bf16),
            pltpu.VMEM((columns, columns), bf16),
            pltpu.VMEM((columns, columns), bf16),
            pltpu.VMEM((columns, columns), bf16),
            pltpu.VMEM((local_rows, columns), bf16),
            pltpu.VMEM((local_rows, columns), bf16),
            pltpu.VMEM((8, experts, 8, 128), f32),
            dma((7,)), dma((7,)),
            dma((chunks,)), dma((chunks,)),
            dma((chunks, 3)), dma((chunks, 3)),
            dma((chunks, 3)), dma((chunks, 3)),
            dma((chunks,)), dma((chunks,)),
        ],
        compiler_params=pltpu.CompilerParams(
            collective_id=0, has_side_effects=True, vmem_limit_bytes=60 * 1024 * 1024
        ),
    )(gradients)


def general(gradients, rows):
    expert_count = gradients.shape[0]
    sums = jnp.sum(jnp.square(gradients.astype(f32)), axis=(1, 2))
    norms = jnp.sqrt(lax.psum(sums, "fsdp"))
    scales = 1.0 / (norms + epsilon)

    def one(pair):
        g, scale = pair
        local = lax.dot_general(g, g, (((0,), (0,)), ((), ())), preferred_element_type=f32)
        raw = lax.psum(local.astype(bf16), "fsdp")
        gram = (raw.astype(f32) * (scale * scale)).astype(bf16)
        current = g
        for it in range(ITERS):
            gf = gram.astype(f32)
            poly = (coef_b * gf + coef_c * mm(gram, gram)).astype(bf16)
            nxt = coef_a * current.astype(f32) + mm(current, poly)
            if it == 0:
                nxt = nxt * scale
            if it < ITERS - 1:
                half = (coef_a * gf + mm(gram, poly)).astype(bf16)
                gram = (coef_a * half.astype(f32) + mm(poly, half)).astype(bf16)
                current = nxt.astype(bf16)
        return (math.sqrt(rows) * nxt).astype(bf16)

    return lax.map(one, (gradients, scales)), norms


def body(gradients, owner):
    expert_count, local_rows, columns = gradients.shape
    fsdp_size = lax.axis_size("fsdp")
    rows = local_rows * fsdp_size
    share = fsdp_size // expert_count
    if fsdp_size == 8 and expert_count == 2 and columns % 1024 == 0 and local_rows % 16 == 0:
        updates, norm_tiles = fused(gradients, rows)
        norms = norm_tiles[:, 0, 0]
    else:
        updates, norms = general(gradients, rows)
    place = lax.axis_index("fsdp") // share
    mine = jnp.sum(jnp.where(owner[0] == place, norms, 0.0))
    slot_rms = (mine / math.sqrt(rows * columns)).reshape(1, 1)
    return updates, slot_rms


def solution(mesh):
    return jax.shard_map(
        body,
        mesh=mesh,
        in_specs=(P("expert", "fsdp", None), P("expert", None)),
        out_specs=(P("expert", "fsdp", None), P("expert", "fsdp")),
        check_vma=False,
    )
```

```python
import functools
import math

import jax
import jax.numpy as jnp
from jax import lax
from jax.experimental import pallas as pl
from jax.experimental.pallas import tpu as pltpu
from jax.sharding import PartitionSpec as P

coef_a = 3.4445
coef_b = -4.775
coef_c = 2.0315
epsilon = 1e-07
ITERS = 3
MESH = pl.DeviceIdType.MESH
f32, bf16 = jnp.float32, jnp.bfloat16


def mm(a, b):
    return jnp.dot(a, b, preferred_element_type=f32)


def kernel(rows, g_ref, out_ref, norm_ref, part, xr, pair, zr, red, gram, poly, half, ping, pong, nb,
           n_send, n_recv, xs_send, xs_recv, zs_send, zs_recv, za_send, za_recv, xa_send, xa_recv):
    experts, local_rows, columns = g_ref.shape
    tile = columns // 4
    piece = tile // 4
    blocks = [(i, j) for i in range(4) for j in range(i, 4)]
    per = len(blocks) // 2
    chunks = experts * per
    size = lax.axis_size("fsdp")
    me = lax.axis_index("fsdp")
    z, x = me // 2, me % 2
    partner = z * 2 + (1 - x)

    barrier = pltpu.get_barrier_semaphore()
    for d in range(1, size):
        pl.semaphore_signal(barrier, inc=1, device_id={"fsdp": (me + d) % size}, device_id_type=MESH)

    def remote(src, dst, send, recv, peer):
        return pltpu.make_async_remote_copy(
            src_ref=src, dst_ref=dst, send_sem=send, recv_sem=recv, device_id={"fsdp": peer}, device_id_type=MESH
        )

    def local_gram(e):
        for i in range(4):
            strip = lax.dot_general(
                g_ref[e, :, tile * i:tile * (i + 1)], g_ref[e, :, tile * i:], (((0,), (0,)), ((), ())),
                preferred_element_type=f32,
            ).astype(bf16)
            for j in range(i, 4):
                part[e, blocks.index((i, j))] = strip[:, tile * (j - i):tile * (j - i + 1)]

    def squares(e):
        total = jnp.zeros((8, 128), f32)
        for n in range(columns // 128):
            value = g_ref[e, :, 128 * n:128 * (n + 1)].astype(f32)
            total = total + jnp.sum((value * value).reshape(local_rows // 8, 8, 128), axis=0)
        nb[0, e] = total

    def x_scatter(k):
        e, c = divmod(k, per)
        return remote(part.at[e, per * (1 - x) + c], xr.at[k], xs_send.at[k], xs_recv.at[k], partner)

    def z_peer(d):
        return (z + d) % 4

    def z_scatter(k, d):
        rows_of = pl.ds(pl.multiple_of(z_peer(d) * piece, piece), piece)
        return remote(pair.at[k, rows_of], zr.at[k, d - 1], zs_send.at[k, d - 1], zs_recv.at[k, d - 1],
                      z_peer(d) * 2 + x)

    mine = pl.ds(pl.multiple_of(z * piece, piece), piece)

    def z_gather(k, d):
        e, c = divmod(k, per)
        slot = red.at[e, per * x + c, mine]
        return remote(slot, slot, za_send.at[k, d - 1], za_recv.at[k, d - 1], z_peer(d) * 2 + x)

    def x_gather(k):
        e, c = divmod(k, per)
        slot = red.at[e, per * x + c]
        return remote(slot, slot, xa_send.at[k], xa_recv.at[k], partner)

    def step_b(k):
        e, c = divmod(k, per)
        x_scatter(k).wait_recv()
        pair[k] = (part[e, per * x + c].astype(f32) + xr[k].astype(f32)).astype(bf16)
        for d in (2, 1, 3):
            z_scatter(k, d).start()

    def step_c(k):
        e, c = divmod(k, per)
        total = pair[k, mine].astype(f32)
        for d in (1, 2, 3):
            z_scatter(k, d).wait_recv()
            total = total + zr[k, d - 1].astype(f32)
        red[e, per * x + c, mine] = total.astype(bf16)
        for d in (2, 1, 3):
            z_gather(k, d).start()

    def step_d(k):
        for d in (1, 2, 3):
            z_gather(k, d).wait_recv()
        x_gather(k).start()
        if k + per < chunks:
            x_scatter(k + per).start()

    def unpack(e, scale):
        for c in range(per):
            x_gather(e * per + c).wait_recv()
        for b, (i, j) in enumerate(blocks):
            block = red[e, b].astype(f32) * (scale * scale)
            gram[tile * i:tile * (i + 1), tile * j:tile * (j + 1)] = block.astype(bf16)
            if i != j:
                gram[tile * j:tile * (j + 1), tile * i:tile * (i + 1)] = block.T.astype(bf16)

    def mirrored(dst, fn):
        for j in range(4):
            cols = slice(tile * j, tile * (j + 1))
            value = fn(tile * (j + 1), cols)
            dst[:tile * (j + 1), cols] = value.astype(bf16)
            for i in range(j):
                span = slice(tile * i, tile * (i + 1))
                dst[cols, span] = value[span].astype(bf16).T

    def stage_poly():
        mirrored(poly, lambda m, cols: coef_b * gram[:m, cols].astype(f32) + coef_c * mm(gram[:m], gram[:, cols]))

    def stage_half():
        mirrored(half, lambda m, cols: coef_a * gram[:m, cols].astype(f32) + mm(gram[:m], poly[:, cols]))

    def stage_gram():
        mirrored(gram, lambda m, cols: coef_a * half[:m, cols].astype(f32) + mm(poly[:m], half[:, cols]))

    def stage_rows(src, dst, factor):
        for n in range(2):
            cols = slice(2 * tile * n, 2 * tile * (n + 1))
            value = coef_a * src[:, cols].astype(f32) + mm(src[...], poly[:, cols])
            if factor is not None:
                value = value * factor
            dst[:, cols] = value.astype(bf16)

    def stages(e, scale):
        root = math.sqrt(rows)
        return [
            functools.partial(unpack, e, scale),
            stage_poly, stage_half, stage_gram,
            functools.partial(stage_rows, g_ref.at[e], ping, scale),
            stage_poly, stage_half, stage_gram,
            functools.partial(stage_rows, ping, pong, None),
            stage_poly,
            functools.partial(stage_rows, pong, out_ref.at[e], root),
        ]

    local_gram(0)
    pl.semaphore_wait(barrier, size - 1)
    for k in range(per):
        x_scatter(k).start()
    for e in range(experts):
        squares(e)

    def norm_copy(d):
        return remote(nb.at[0], nb.at[d], n_send.at[d - 1], n_recv.at[d - 1], (me + d) % size)

    for d in range(1, size):
        norm_copy(d).start()
    local_gram(1)

    scales = []

    def finish_norms():
        total = nb[0]
        for d in range(1, size):
            norm_copy(d).wait_recv()
            total = total + nb[d]
        for e in range(experts):
            norm = jnp.sqrt(jnp.sum(total[e], keepdims=True))
            norm_ref[e] = jnp.broadcast_to(norm, (8, 128))
            scales.append(1.0 / (norm + epsilon))

    work = []
    for t in range(chunks + 2):
        if t < chunks:
            step_b(t)
        if 0 <= t - 1 < chunks:
            step_c(t - 1)
        if 0 <= t - 2 < chunks:
            step_d(t - 2)
        if t == per:
            finish_norms()
            work = stages(0, scales[0])
        if t >= per + 2:
            for _ in range(3):
                if work:
                    work.pop(0)()
    while work:
        work.pop(0)()
    for stage in stages(1, scales[1]):
        stage()

    for k in range(chunks):
        x_scatter(k).wait_send()
        x_gather(k).wait_send()
        for d in (1, 2, 3):
            z_scatter(k, d).wait_send()
            z_gather(k, d).wait_send()
    for d in range(1, size):
        norm_copy(d).wait_send()


def fused(gradients, rows):
    experts, local_rows, columns = gradients.shape
    tile = columns // 4
    chunks = experts * 5
    dma = pltpu.SemaphoreType.DMA
    vmem = pl.BlockSpec(memory_space=pltpu.VMEM)
    return pl.pallas_call(
        functools.partial(kernel, rows),
        out_shape=(
            jax.ShapeDtypeStruct(gradients.shape, bf16),
            jax.ShapeDtypeStruct((experts, 8, 128), f32),
        ),
        in_specs=[vmem],
        out_specs=(vmem, vmem),
        scratch_shapes=[
            pltpu.VMEM((experts, 10, tile, tile), bf16),
            pltpu.VMEM((chunks, tile, tile), bf16),
            pltpu.VMEM((chunks, tile, tile), bf16),
            pltpu.VMEM((chunks, 3, tile // 4, tile), bf16),
            pltpu.VMEM((experts, 10, tile, tile), bf16),
            pltpu.VMEM((columns, columns), bf16),
            pltpu.VMEM((columns, columns), bf16),
            pltpu.VMEM((columns, columns), bf16),
            pltpu.VMEM((local_rows, columns), bf16),
            pltpu.VMEM((local_rows, columns), bf16),
            pltpu.VMEM((8, experts, 8, 128), f32),
            dma((7,)), dma((7,)),
            dma((chunks,)), dma((chunks,)),
            dma((chunks, 3)), dma((chunks, 3)),
            dma((chunks, 3)), dma((chunks, 3)),
            dma((chunks,)), dma((chunks,)),
        ],
        compiler_params=pltpu.CompilerParams(
            collective_id=0, has_side_effects=True, vmem_limit_bytes=60 * 1024 * 1024
        ),
    )(gradients)


def general(gradients, rows):
    expert_count = gradients.shape[0]
    sums = jnp.sum(jnp.square(gradients.astype(f32)), axis=(1, 2))
    norms = jnp.sqrt(lax.psum(sums, "fsdp"))
    scales = 1.0 / (norms + epsilon)

    def one(pair):
        g, scale = pair
        local = lax.dot_general(g, g, (((0,), (0,)), ((), ())), preferred_element_type=f32)
        raw = lax.psum(local.astype(bf16), "fsdp")
        gram = (raw.astype(f32) * (scale * scale)).astype(bf16)
        current = g
        for it in range(ITERS):
            gf = gram.astype(f32)
            poly = (coef_b * gf + coef_c * mm(gram, gram)).astype(bf16)
            nxt = coef_a * current.astype(f32) + mm(current, poly)
            if it == 0:
                nxt = nxt * scale
            if it < ITERS - 1:
                half = (coef_a * gf + mm(gram, poly)).astype(bf16)
                gram = (coef_a * half.astype(f32) + mm(poly, half)).astype(bf16)
                current = nxt.astype(bf16)
        return (math.sqrt(rows) * nxt).astype(bf16)

    return lax.map(one, (gradients, scales)), norms


def body(gradients, owner):
    expert_count, local_rows, columns = gradients.shape
    fsdp_size = lax.axis_size("fsdp")
    rows = local_rows * fsdp_size
    share = fsdp_size // expert_count
    if fsdp_size == 8 and expert_count == 2 and columns % 1024 == 0 and local_rows % 16 == 0:
        updates, norm_tiles = fused(gradients, rows)
        norms = norm_tiles[:, 0, 0]
    else:
        updates, norms = general(gradients, rows)
    place = lax.axis_index("fsdp") // share
    mine = jnp.sum(jnp.where(owner[0] == place, norms, 0.0))
    slot_rms = (mine / math.sqrt(rows * columns)).reshape(1, 1)
    return updates, slot_rms


def solution(mesh):
    return jax.shard_map(
        body,
        mesh=mesh,
        in_specs=(P("expert", "fsdp", None), P("expert", None)),
        out_specs=(P("expert", "fsdp", None), P("expert", "fsdp")),
        check_vma=False,
    )
```
